32 devices in a mesh: grp: 4 (over x, core), ctx: 8 (over z, y).
Axes of the slice: x: 2, y: 2, z: 4, core: 2. Of those that a mesh axis runs over, the one named last changes fastest.
Arguments:
- queries: bfloat16 [4096, 4096], P(('grp', 'ctx')), parts along dimension 0, may hold values from -8 to 8
- key_states: bfloat16 [4096, 512], P(('grp', 'ctx')), parts along dimension 0, may hold values from -8 to 8
- value_states: bfloat16 [4096, 512], P(('grp', 'ctx')), parts along dimension 0, may hold values from -6 to 6
- grads_out: bfloat16 [4096, 4096], P(('grp', 'ctx')), parts along dimension 0, may hold values from -6 to 6
- doc_lengths: int32 [32], P('grp'), parts along dimension 0, may hold values from 1 to 256, as said below
- block_plan: int32 [64], P('grp'), parts along dimension 0, may hold values from 0 to 15, as said below
- needed: int32 [32, 2], P('grp'), parts along dimension 0, may hold values from 0 to 15, as said below
Outputs:
- outputs: bfloat16 [4096, 4096], P(('grp', 'ctx')), parts along dimension 0
- query_grads: bfloat16 [4096, 4096], P(('grp', 'ctx')), parts along dimension 0
- key_grads: bfloat16 [4096, 512], P(('grp', 'ctx')), parts along dimension 0
- value_grads: bfloat16 [4096, 512], P(('grp', 'ctx')), parts along dimension 0
The draws below stay inside these ranges and needn't reach their ends.
There are 4 independent parts, one for each index of `grp`. The reference program is written for one: setup_inputs(seed, part) draws one part's arguments, and reference() takes and returns one part's arrays. A program takes and returns all parts, laid end to end along the dimension named above; each array names one. Nothing has to cross between parts.
Inputs may be any that keep to these rules, and one draw needn't show every extreme that they name: `doc_lengths`: the lengths sum to 1024 and one of them is exactly 256. `block_plan`: each block position appears once. `needed`: each row lists 2 different stored block numbers, no two of which have the same value of block number // 2.
All inputs are finite; a program needn't handle non-finite values.
Results may differ from the reference program's by a relative error of at most 0.013.
Values may be sent and summed in bfloat16 or wider, within the bound.
A program may use at most 128 MiB of HBM per device.

```python
import math
import jax
import jax.numpy as jnp
from jax import lax

HEADS = 32
KV_HEADS = 4
HEAD_DIM = 128
BLK = 64
NDOC = 8
TOK_DEV = 128
NBLK = 16
TOKENS = 1024
NEED = 2
N_CTX = 8


def plan_parts(key):
    base = jax.random.fold_in(key, 7001)
    big_key, weight_key, plan_key, rank_key = jax.random.split(base, 4)
    doc_slots = jnp.arange(NDOC, dtype=jnp.int32)
    big_doc = jax.random.randint(big_key, (), 0, NDOC, dtype=jnp.int32)
    weights = jnp.where(doc_slots == big_doc, 0, jax.random.randint(weight_key, (NDOC,), 2, 5, dtype=jnp.int32))
    remaining = TOKENS - TOKENS // 4
    shares = remaining * weights // jnp.sum(weights)
    shares = shares + jnp.where(doc_slots == (big_doc + 1) % NDOC, remaining - jnp.sum(shares), 0)
    lengths = jnp.where(doc_slots == big_doc, TOKENS // 4, shares).astype(jnp.int32)
    plan = jax.random.permutation(plan_key, NBLK).astype(jnp.int32)
    return (lengths, plan, rank_key)


def draw_queries(key, part):
    normal_key = jax.random.fold_in(jax.random.fold_in(key, 11), 0)
    sampled = jnp.clip(jax.random.normal(normal_key, (TOKENS, HEADS * HEAD_DIM), jnp.float32), -6.0, 6.0)
    return sampled.astype(jnp.bfloat16)


def draw_key_states(key, part):
    sampled = jnp.clip(jax.random.normal(jax.random.fold_in(key, 13), (TOKENS, KV_HEADS * HEAD_DIM), jnp.float32), -6.0, 6.0)
    return sampled.astype(jnp.bfloat16)


def draw_doc_lengths(key, part):
    lengths, plan, rank_key = plan_parts(key)
    return lengths


def draw_block_plan(key, part):
    lengths, plan, rank_key = plan_parts(key)
    return plan


def draw_needed(key, part):
    lengths, plan, rank_key = plan_parts(key)
    ends = jnp.cumsum(lengths).astype(jnp.int32)

    def doc_of(points):
        return jnp.sum((ends[None, :] <= points[:, None]).astype(jnp.int32), axis=1)
    first_doc = doc_of(plan * BLK)
    last_doc = doc_of(plan * BLK + BLK - 1)
    owners = NBLK // 2
    owner_ids = jnp.arange(owners, dtype=jnp.int32)
    query_blocks = jnp.stack([2 * owner_ids, 2 * owner_ids + 1], axis=1)
    query_plan = jnp.take(plan, query_blocks)
    query_first = jnp.take(first_doc, query_blocks)
    useful = (plan[None, None, :] < query_plan[:, :, None]) & (last_doc[None, None, :] == query_first[:, :, None])
    useful = jnp.any(useful, axis=1)
    ranks = jax.vmap(lambda row_key: jax.random.permutation(row_key, NBLK))(jax.random.split(rank_key, owners))
    score = useful.astype(jnp.int32) * NBLK + ranks.astype(jnp.int32)
    paired = score.reshape(owners, owners, 2)
    second = (paired[:, :, 1] > paired[:, :, 0]).astype(jnp.int32)
    owner_score = jnp.max(paired, axis=2)
    owner_block = 2 * owner_ids[None, :] + second
    order = jnp.argsort(-owner_score, axis=1, stable=True)[:, :NEED]
    return jnp.take_along_axis(owner_block, order, axis=1).astype(jnp.int32)


def steps_of(rng, shape, shards, low, top_value):
    gain = 1.0
    for position, shards_of in shards:
        steps = jax.random.uniform(jax.random.fold_in(jax.random.fold_in(rng, 6), position), (shards_of,), jnp.float32, low / len(shards), top_value / len(shards))
        gain = gain * jnp.repeat(jnp.exp(steps), shape[position] // shards_of).reshape((-1,) + (1,) * (len(shape) - 1 - position))
    return gain


def noise(key, extent, scale, bound, cuts=(), held_as=jnp.bfloat16):
    values = scale * jax.random.normal(key, extent, jnp.float32)
    if cuts:
        values = values * steps_of(key, extent, cuts, -0.22, 0.18)
    return jnp.clip(values, -bound, bound).astype(held_as)


def setup_inputs(seed: int = 0, part: int = 0) -> dict:
    key_list = jax.random.split(jax.random.key(seed), 8)
    part_splits = jax.random.split(jax.random.fold_in(key_list[7], part), 8)
    queries = draw_queries(jax.random.fold_in(jax.random.fold_in(key_list[7], part), 71), part)
    key_states = draw_key_states(jax.random.fold_in(jax.random.fold_in(key_list[7], part), 71), part)
    value_states = noise(part_splits[2], (TOKENS, KV_HEADS * HEAD_DIM), 1.0, 6.0, ((0, 8),))
    grads_out = noise(part_splits[3], (TOKENS, HEADS * HEAD_DIM), 1.0, 6.0, ((0, 8),))
    doc_lengths = draw_doc_lengths(jax.random.fold_in(jax.random.fold_in(key_list[7], part), 71), part)
    block_plan = draw_block_plan(jax.random.fold_in(jax.random.fold_in(key_list[7], part), 71), part)
    needed = draw_needed(jax.random.fold_in(jax.random.fold_in(key_list[7], part), 71), part)
    return dict(queries=queries, key_states=key_states, value_states=value_states, grads_out=grads_out, doc_lengths=doc_lengths, block_plan=block_plan, needed=needed)


masked_score = -1e+30

def token_labels(block_plan, doc_ends):
    stored = jnp.arange(TOKENS, dtype=jnp.int32)
    stored_block = stored // BLK
    placed = jnp.take(block_plan, stored_block).astype(jnp.int32) * BLK + stored % BLK
    documents = lax.optimization_barrier(jnp.sum((doc_ends[None, :] <= placed[:, None]).astype(jnp.int32), axis=1))
    return (stored_block, placed, documents)

def reference(queries, key_states, value_states, grads_out, doc_lengths, block_plan, needed):
    score_scale = 1.0 / math.sqrt(HEAD_DIM)
    group_heads = HEADS // KV_HEADS
    doc_ends = jnp.cumsum(doc_lengths).astype(jnp.int32)
    key_block, key_place, key_doc = token_labels(block_plan, doc_ends)
    keys_grouped = key_states.astype(jnp.float32).reshape(TOKENS, KV_HEADS, HEAD_DIM)
    values_grouped = value_states.astype(jnp.float32).reshape(TOKENS, KV_HEADS, HEAD_DIM)

    def per_rank(carried, inputs):
        key_sum, value_sum = carried
        rank_queries, rank_grads, wanted, own_rank = inputs
        first_row = own_rank * TOK_DEV
        query_block = lax.dynamic_slice_in_dim(key_block, first_row, TOK_DEV)
        query_place = lax.dynamic_slice_in_dim(key_place, first_row, TOK_DEV)
        query_doc = lax.dynamic_slice_in_dim(key_doc, first_row, TOK_DEV)
        listed = jnp.any(wanted[:, None] == key_block[None, :], axis=0)
        allowed = listed[None, :] | (query_block[:, None] == key_block[None, :])
        visible_pairs = allowed & (query_doc[:, None] == key_doc[None, :]) & (key_place[None, :] <= query_place[:, None])
        grouped = rank_queries.astype(jnp.float32).reshape(TOK_DEV, KV_HEADS, group_heads, HEAD_DIM)
        scores = jnp.einsum('qhgd,khd->hgqk', grouped, keys_grouped) * score_scale
        scores = jnp.where(visible_pairs, scores, masked_score)
        highest = lax.optimization_barrier(jnp.max(scores, axis=-1))
        totals = lax.optimization_barrier(jnp.sum(jnp.where(visible_pairs, jnp.exp(scores - highest[..., None]), 0.0), axis=-1))
        log_total = highest + jnp.log(totals)
        soft_weights = jnp.where(visible_pairs, jnp.exp(scores - log_total[..., None]), 0.0)
        probs_low = lax.optimization_barrier(soft_weights.astype(jnp.bfloat16)).astype(jnp.float32)
        attended = jnp.einsum('hgqk,khd->qhgd', soft_weights, values_grouped)
        outputs = attended.reshape(TOK_DEV, HEADS * HEAD_DIM).astype(jnp.bfloat16)
        gradient_rows = rank_grads.astype(jnp.float32).reshape(TOK_DEV, KV_HEADS, group_heads, HEAD_DIM)
        products = gradient_rows * outputs.astype(jnp.float32).reshape(TOK_DEV, KV_HEADS, group_heads, HEAD_DIM)
        row_delta = jnp.transpose(lax.optimization_barrier(jnp.sum(products, axis=-1)), (1, 2, 0))
        prob_grads = jnp.einsum('qhgd,khd->hgqk', gradient_rows, values_grouped)
        score_grads = (soft_weights * (prob_grads - row_delta[..., None])).astype(jnp.bfloat16)
        score_grads = lax.optimization_barrier(score_grads).astype(jnp.float32)
        query_part = jnp.einsum('hgqk,khd->qhgd', score_grads, keys_grouped) * score_scale
        query_grads = query_part.reshape(TOK_DEV, HEADS * HEAD_DIM).astype(jnp.bfloat16)
        key_part = jnp.einsum('hgqk,qhgd->khd', score_grads, grouped) * score_scale
        value_part = jnp.einsum('hgqk,qhgd->khd', probs_low, gradient_rows)
        key_low = lax.optimization_barrier(key_part.reshape(TOKENS, -1).astype(jnp.bfloat16))
        value_low = lax.optimization_barrier(value_part.reshape(TOKENS, -1).astype(jnp.bfloat16))
        key_sum = key_sum + key_low.astype(jnp.float32)
        value_sum = value_sum + value_low.astype(jnp.float32)
        return ((key_sum, value_sum), (outputs, query_grads))
    empty_sum = jnp.zeros((TOKENS, KV_HEADS * HEAD_DIM), jnp.float32)
    inputs = (queries.reshape(N_CTX, TOK_DEV, HEADS * HEAD_DIM), grads_out.reshape(N_CTX, TOK_DEV, HEADS * HEAD_DIM), needed, jnp.arange(N_CTX, dtype=jnp.int32))
    sums, stacked = lax.scan(per_rank, (empty_sum, empty_sum), inputs)
    outputs = stacked[0].reshape(TOKENS, HEADS * HEAD_DIM)
    query_grads = stacked[1].reshape(TOKENS, HEADS * HEAD_DIM)
    return (outputs, query_grads, sums[0].astype(jnp.bfloat16), sums[1].astype(jnp.bfloat16))
```

```python
import functools
import math

import jax
import jax.numpy as jnp
from jax import lax
from jax.experimental import pallas as pl
from jax.experimental.pallas import tpu as pltpu
from jax.sharding import PartitionSpec as P

HEADS = 32
KV_HEADS = 4
HEAD_DIM = 128
BLK = 64
GROUP = HEADS // KV_HEADS
CHUNKS = 2
PER_CHUNK = KV_HEADS // CHUNKS
WIDE = 2 * HEAD_DIM * PER_CHUNK
PAIR = 2

masked_score = -1e30


def matmul(a, b, contract):
    return lax.dot_general(
        a, b, ((contract[:1], contract[1:]), ((), ())), preferred_element_type=jnp.float32
    )


def kernel(n, q_hbm, k_ref, v_ref, do_hbm, doc_ref, plan_ref, need_ref, *rest):
    out_hbm, dq_hbm, dk_ref, dv_ref = rest[:4]
    q_buf, do_buf, out_buf, dq_buf, key_acc, value_acc, bias = rest[4:11]
    send, grad_send, grad_recv = rest[11:14]
    recv = rest[14 : 14 + CHUNKS]
    fwd_send, fwd_recv, bwd_send, bwd_recv, load_sem, store_sem = rest[14 + CHUNKS :]
    rows = q_buf.shape[0]
    own_blocks = rows // BLK
    listed_count = need_ref.shape[1]
    me = lax.axis_index("ctx")
    score_scale = 1.0 / math.sqrt(HEAD_DIM)
    chunk_cols = PER_CHUNK * GROUP * HEAD_DIM

    def cols(c):
        return pl.ds(c * chunk_cols, chunk_cols)

    loads, stores, fetches, returns = {}, {}, {}, {}
    for c in range(CHUNKS):
        for i, (src, dst) in enumerate(((q_hbm, q_buf), (do_hbm, do_buf))):
            loads[i, c] = pltpu.make_async_copy(
                src.at[:, cols(c)], dst.at[:, cols(c)], load_sem.at[i, c]
            )
            loads[i, c].start()

    barrier = pltpu.get_barrier_semaphore()
    for o in range(1, n):
        pl.semaphore_signal(
            barrier,
            inc=1,
            device_id={"ctx": lax.rem(me + o, n)},
            device_id_type=pl.DeviceIdType.MESH,
        )

    for o in range(1, n):
        peer = lax.rem(me + o, n)
        half = jnp.int32(0)
        for j in range(listed_count):
            block = need_ref[peer, j]
            half = jnp.where(block // own_blocks == me, block % own_blocks, half)
        keys, values = k_ref[half], v_ref[half]
        for c in range(CHUNKS):
            for i in range(PER_CHUNK):
                g = c * PER_CHUNK + i
                at = slice(g * HEAD_DIM, (g + 1) * HEAD_DIM)
                base = 2 * i * HEAD_DIM
                send[o, c, :, base : base + HEAD_DIM] = keys[:, at]
                send[o, c, :, base + HEAD_DIM : base + 2 * HEAD_DIM] = values[:, at]
    for c in range(CHUNKS):
        recv[c][0] = jnp.zeros((BLK, WIDE), jnp.bfloat16)

    pl.semaphore_wait(barrier, n - 1)
    for c in range(CHUNKS):
        for o in range(1, n):
            fetches[o, c] = pltpu.make_async_remote_copy(
                src_ref=send.at[o, c],
                dst_ref=recv[c].at[o],
                send_sem=fwd_send.at[o, c],
                recv_sem=fwd_recv.at[o, c],
                device_id={"ctx": lax.rem(me + o, n)},
                device_id_type=pl.DeviceIdType.MESH,
            )
            fetches[o, c].start()

    ends, total = [], jnp.int32(0)
    for d in range(doc_ref.shape[0]):
        total = total + doc_ref[d]
        ends.append(total)

    def documents(place):
        doc = jnp.zeros_like(place)
        for end in ends:
            doc = doc + (place >= end).astype(jnp.int32)
        return doc

    key_row = lax.broadcasted_iota(jnp.int32, (BLK, rows), 0)
    query_col = lax.broadcasted_iota(jnp.int32, (BLK, rows), 1)
    query_local = query_col // BLK
    query_place = query_col
    for b in range(own_blocks):
        shift = (plan_ref[me * own_blocks + b] - b) * BLK
        query_place = jnp.where(query_local == b, query_col + shift, query_place)
    query_doc = documents(query_place)
    listed = [need_ref[me, j] for j in range(listed_count)]
    for s in range(own_blocks + listed_count):
        if s < own_blocks:
            block = me * own_blocks + s
            found = jnp.int32(0)
            for b in listed:
                found = jnp.where(b == block, 1, found)
            allowed = jnp.where(query_local == s, 1, found)
        else:
            block = listed[s - own_blocks]
            allowed = jnp.where(block // own_blocks == me, 0, jnp.ones_like(query_col))
        key_place = key_row + plan_ref[block] * BLK
        visible = (allowed > 0) & (documents(key_place) == query_doc) & (key_place <= query_place)
        bias[s * BLK : (s + 1) * BLK, :] = jnp.where(visible, 0.0, masked_score)

    slots = [lax.rem(me - b // own_blocks + n, n) for b in listed]
    exponent = score_scale * math.log2(math.e)

    for c in range(CHUNKS):
        loads[0, c].wait()
        loads[1, c].wait()
        for o in range(1, n):
            fetches[o, c].wait_recv()
        arrived = [recv[c][slot] for slot in slots]
        for i in range(PER_CHUNK):
            g = c * PER_CHUNK + i
            own_at = slice(g * HEAD_DIM, (g + 1) * HEAD_DIM)
            base = 2 * i * HEAD_DIM
            keys = jnp.concatenate(
                [k_ref[b, :, own_at] for b in range(own_blocks)]
                + [piece[:, base : base + HEAD_DIM] for piece in arrived],
                axis=0,
            )
            values = jnp.concatenate(
                [v_ref[b, :, own_at] for b in range(own_blocks)]
                + [piece[:, base + HEAD_DIM : base + 2 * HEAD_DIM] for piece in arrived],
                axis=0,
            )
            keys_t, values_t = keys.T, values.T
            key_grad = value_grad = None
            for p in range(GROUP // PAIR):
                heads = [
                    slice((g * GROUP + p * PAIR + x) * HEAD_DIM, (g * GROUP + p * PAIR + x + 1) * HEAD_DIM)
                    for x in range(PAIR)
                ]
                queries = jnp.concatenate([q_buf[:, at] for at in heads], axis=0)
                grads = jnp.concatenate([do_buf[:, at] for at in heads], axis=0)
                mask = bias[...]
                scores = matmul(keys, queries, (1, 1)) + jnp.concatenate([mask] * PAIR, axis=1)
                highest = jnp.max(scores, axis=0, keepdims=True)
                weights = jnp.exp2((scores - highest) * exponent)
                weights = weights * (1.0 / jnp.sum(weights, axis=0, keepdims=True))
                low = weights.astype(jnp.bfloat16)
                attended = matmul(values_t, low, (1, 0)).T.astype(jnp.bfloat16)
                prob_grads = matmul(values, grads, (1, 1))
                delta = jnp.sum(weights * prob_grads, axis=0, keepdims=True)
                score_grads = (weights * (prob_grads - delta)).astype(jnp.bfloat16)
                query_grad = (matmul(keys_t, score_grads, (1, 0)) * score_scale).T
                query_grad = query_grad.astype(jnp.bfloat16)
                for x, at in enumerate(heads):
                    out_buf[:, at] = attended[x * rows : (x + 1) * rows]
                    dq_buf[:, at] = query_grad[x * rows : (x + 1) * rows]
                more_keys = matmul(score_grads, queries, (1, 0))
                more_values = matmul(low, grads, (1, 0))
                key_grad = more_keys if key_grad is None else key_grad + more_keys
                value_grad = more_values if value_grad is None else value_grad + more_values
            key_grad = key_grad * score_scale
            key_acc[:, own_at] = key_grad[:rows]
            value_acc[:, own_at] = value_grad[:rows]
            for o in range(1, n):
                owner = lax.rem(me - o + n, n)
                for grad, at in ((key_grad, base), (value_grad, base + HEAD_DIM)):
                    piece = jnp.zeros((BLK, HEAD_DIM), jnp.float32)
                    for j, block in enumerate(listed):
                        first = rows + j * BLK
                        piece = jnp.where(
                            block // own_blocks == owner, grad[first : first + BLK], piece
                        )
                    grad_send[o, c, :, at : at + HEAD_DIM] = piece.astype(jnp.bfloat16)
        for o in range(1, n):
            returns[o, c] = pltpu.make_async_remote_copy(
                src_ref=grad_send.at[o, c],
                dst_ref=grad_recv.at[o, c],
                send_sem=bwd_send.at[o, c],
                recv_sem=bwd_recv.at[o, c],
                device_id={"ctx": lax.rem(me - o + n, n)},
                device_id_type=pl.DeviceIdType.MESH,
            )
            returns[o, c].start()
        for i, (src, dst) in enumerate(((out_buf, out_hbm), (dq_buf, dq_hbm))):
            stores[i, c] = pltpu.make_async_copy(
                src.at[:, cols(c)], dst.at[:, cols(c)], store_sem.at[i, c]
            )
            stores[i, c].start()

    for c in range(CHUNKS):
        for o in range(1, n):
            returns[o, c].wait_recv()
        for i in range(PER_CHUNK):
            g = c * PER_CHUNK + i
            own_at = slice(g * HEAD_DIM, (g + 1) * HEAD_DIM)
            base = 2 * i * HEAD_DIM
            for acc, result, at in ((key_acc, dk_ref, base), (value_acc, dv_ref, base + HEAD_DIM)):
                sums = [acc[b * BLK : (b + 1) * BLK, own_at] for b in range(own_blocks)]
                for o in range(1, n):
                    peer = lax.rem(me + o, n)
                    part = grad_recv[o, c, :, at : at + HEAD_DIM].astype(jnp.float32)
                    for b in range(own_blocks):
                        hit = jnp.int32(0)
                        for j in range(listed_count):
                            hit = jnp.where(need_ref[peer, j] == me * own_blocks + b, 1, hit)
                        sums[b] = sums[b] + jnp.where(hit > 0, part, 0.0)
                for b in range(own_blocks):
                    result[b * BLK : (b + 1) * BLK, own_at] = sums[b].astype(jnp.bfloat16)
    for c in range(CHUNKS):
        for o in range(1, n):
            fetches[o, c].wait_send()
            returns[o, c].wait_send()
        stores[0, c].wait()
        stores[1, c].wait()


def on_device(queries, key_states, value_states, grads_out, doc_lengths, block_plan, needed):
    n = lax.axis_size("ctx")
    rows, width = queries.shape
    kv_width = key_states.shape[1]
    blocked = (rows // BLK, BLK, kv_width)
    key_count = rows + needed.shape[1] * BLK
    vmem = pl.BlockSpec(memory_space=pltpu.VMEM)
    smem = pl.BlockSpec(memory_space=pltpu.SMEM)
    anywhere = pl.BlockSpec(memory_space=pl.ANY)
    wide = jax.ShapeDtypeStruct((rows, width), jnp.bfloat16)
    narrow = jax.ShapeDtypeStruct((rows, kv_width), jnp.bfloat16)
    exchange = pltpu.VMEM((n, CHUNKS, BLK, WIDE), jnp.bfloat16)
    dma = pltpu.SemaphoreType.DMA
    return pl.pallas_call(
        functools.partial(kernel, n),
        out_shape=(wide, wide, narrow, narrow),
        in_specs=[anywhere, vmem, vmem, anywhere, smem, smem, smem],
        out_specs=(anywhere, anywhere, vmem, vmem),
        scratch_shapes=[pltpu.VMEM((rows, width), jnp.bfloat16)] * 4
        + [pltpu.VMEM((rows, kv_width), jnp.float32)] * 2
        + [pltpu.VMEM((key_count, rows), jnp.float32)]
        + [exchange] * 3
        + [pltpu.VMEM((n, BLK, WIDE), jnp.bfloat16)] * CHUNKS
        + [dma((n, CHUNKS))] * 4
        + [dma((2, CHUNKS))] * 2,
        compiler_params=pltpu.CompilerParams(collective_id=0, has_side_effects=True),
    )(
        queries,
        key_states.reshape(blocked),
        value_states.reshape(blocked),
        grads_out,
        doc_lengths,
        block_plan,
        needed,
    )


def solution(mesh):
    tokens = P(("grp", "ctx"), None)
    return jax.shard_map(
        on_device,
        mesh=mesh,
        in_specs=(tokens, tokens, tokens, tokens, P("grp"), P("grp"), P("grp", None)),
        out_specs=(tokens, tokens, tokens, tokens),
        check_vma=False,
    )
```

```python
import functools
import math

import jax
import jax.numpy as jnp
from jax import lax
from jax.experimental import pallas as pl
from jax.experimental.pallas import tpu as pltpu
from jax.sharding import PartitionSpec as P

HEADS = 32
KV_HEADS = 4
HEAD_DIM = 128
BLK = 64
GROUP = HEADS // KV_HEADS
CHUNKS = 2
PER_CHUNK = KV_HEADS // CHUNKS
WIDE = 2 * HEAD_DIM * PER_CHUNK
PAIR = 2

masked_score = -1e30


def matmul(a, b, contract):
    return lax.dot_general(
        a, b, ((contract[:1], contract[1:]), ((), ())), preferred_element_type=jnp.float32
    )


def kernel(n, q_hbm, k_ref, v_ref, do_hbm, doc_ref, plan_ref, need_ref, *rest):
    out_hbm, dq_hbm, dk_ref, dv_ref = rest[:4]
    q_buf, do_buf, out_buf, dq_buf, key_acc, value_acc, bias = rest[4:11]
    send, grad_send, grad_recv = rest[11:14]
    recv = rest[14 : 14 + CHUNKS]
    relayed = rest[14 + CHUNKS : 14 + 2 * CHUNKS]
    whole = rest[14 + 2 * CHUNKS]
    fwd_send, fwd_recv, bwd_send, bwd_recv, load_sem, store_sem = rest[15 + 2 * CHUNKS :]
    rows = q_buf.shape[0]
    own_blocks = rows // BLK
    listed_count = need_ref.shape[1]
    me = lax.axis_index("ctx")
    side = n // 2
    local = lax.rem(me, side)
    side_start = me - local
    partner = lax.rem(me + side, n)
    score_scale = 1.0 / math.sqrt(HEAD_DIM)
    chunk_cols = PER_CHUNK * GROUP * HEAD_DIM

    def cols(c):
        return pl.ds(c * chunk_cols, chunk_cols)

    loads, stores, fetches, returns = {}, {}, {}, {}
    for c in range(CHUNKS):
        for i, (src, dst) in enumerate(((q_hbm, q_buf), (do_hbm, do_buf))):
            loads[i, c] = pltpu.make_async_copy(
                src.at[:, cols(c)], dst.at[:, cols(c)], load_sem.at[i, c]
            )
            loads[i, c].start()

    barrier = pltpu.get_barrier_semaphore()
    for o in range(1, n):
        pl.semaphore_signal(
            barrier,
            inc=1,
            device_id={"ctx": lax.rem(me + o, n)},
            device_id_type=pl.DeviceIdType.MESH,
        )

    def near(o):
        return side_start + lax.rem(local + o, side)

    def half_for(peer, owner):
        half = jnp.int32(0)
        for j in range(listed_count):
            block = need_ref[peer, j]
            half = jnp.where(block // own_blocks == owner, block % own_blocks, half)
        return half

    def pack(keys, values, c):
        pieces = []
        for i in range(PER_CHUNK):
            g = c * PER_CHUNK + i
            at = slice(g * HEAD_DIM, (g + 1) * HEAD_DIM)
            pieces += [keys[:, at], values[:, at]]
        return jnp.concatenate(pieces, axis=1)

    def fetch(key, src, dst, peer, slot, c):
        fetches[key] = pltpu.make_async_remote_copy(
            src_ref=src,
            dst_ref=dst,
            send_sem=fwd_send.at[slot, c],
            recv_sem=fwd_recv.at[slot, c],
            device_id={"ctx": peer},
            device_id_type=pl.DeviceIdType.MESH,
        )
        fetches[key].start()

    for c in range(CHUNKS):
        for b in range(own_blocks):
            whole[c, b] = pack(k_ref[b], v_ref[b], c)
    for o in range(1, side):
        half = half_for(near(o), me)
        keys, values = k_ref[half], v_ref[half]
        for c in range(CHUNKS):
            send[o, c] = pack(keys, values, c)
    for c in range(CHUNKS):
        recv[c][0] = jnp.zeros((BLK, WIDE), jnp.bfloat16)

    pl.semaphore_wait(barrier, n - 1)
    for c in range(CHUNKS):
        fetch((0, c), whole.at[c], relayed[c], partner, 0, c)
    for c in range(CHUNKS):
        for o in range(1, side):
            fetch((o, c), send.at[o, c], recv[c].at[o], near(o), o, c)

    ends, total = [], jnp.int32(0)
    for d in range(doc_ref.shape[0]):
        total = total + doc_ref[d]
        ends.append(total)

    def documents(place):
        doc = jnp.zeros_like(place)
        for end in ends:
            doc = doc + (place >= end).astype(jnp.int32)
        return doc

    key_row = lax.broadcasted_iota(jnp.int32, (BLK, rows), 0)
    query_col = lax.broadcasted_iota(jnp.int32, (BLK, rows), 1)
    query_local = query_col // BLK
    query_place = query_col
    for b in range(own_blocks):
        shift = (plan_ref[me * own_blocks + b] - b) * BLK
        query_place = jnp.where(query_local == b, query_col + shift, query_place)
    query_doc = documents(query_place)
    listed = [need_ref[me, j] for j in range(listed_count)]
    for s in range(own_blocks + listed_count):
        if s < own_blocks:
            block = me * own_blocks + s
            found = jnp.int32(0)
            for b in listed:
                found = jnp.where(b == block, 1, found)
            allowed = jnp.where(query_local == s, 1, found)
        else:
            block = listed[s - own_blocks]
            allowed = jnp.where(block // own_blocks == me, 0, jnp.ones_like(query_col))
        key_place = key_row + plan_ref[block] * BLK
        visible = (allowed > 0) & (documents(key_place) == query_doc) & (key_place <= query_place)
        bias[s * BLK : (s + 1) * BLK, :] = jnp.where(visible, 0.0, masked_score)

    for c in range(CHUNKS):
        fetches[0, c].wait_recv()
        for o in range(1, side):
            send[side + o, c] = relayed[c][half_for(near(o), partner)]
            fetch((side + o, c), send.at[side + o, c], recv[c].at[side + o], near(o), side + o, c)
        recv[c][side] = relayed[c][half_for(me, partner)]

    slots = []
    for b in listed:
        owner = b // own_blocks
        owner_local = owner % side
        apart = jnp.where(owner - owner_local == side_start, 0, side)
        slots.append(lax.rem(local - owner_local + side, side) + apart)
    exponent = score_scale * math.log2(math.e)

    for c in range(CHUNKS):
        loads[0, c].wait()
        loads[1, c].wait()
        for o in range(1, n):
            if o != side:
                fetches[o, c].wait_recv()
        arrived = [recv[c][slot] for slot in slots]
        for i in range(PER_CHUNK):
            g = c * PER_CHUNK + i
            own_at = slice(g * HEAD_DIM, (g + 1) * HEAD_DIM)
            base = 2 * i * HEAD_DIM
            keys = jnp.concatenate(
                [k_ref[b, :, own_at] for b in range(own_blocks)]
                + [piece[:, base : base + HEAD_DIM] for piece in arrived],
                axis=0,
            )
            values = jnp.concatenate(
                [v_ref[b, :, own_at] for b in range(own_blocks)]
                + [piece[:, base + HEAD_DIM : base + 2 * HEAD_DIM] for piece in arrived],
                axis=0,
            )
            keys_t, values_t = keys.T, values.T
            key_grad = value_grad = None
            for p in range(GROUP // PAIR):
                heads = [
                    slice((g * GROUP + p * PAIR + x) * HEAD_DIM, (g * GROUP + p * PAIR + x + 1) * HEAD_DIM)
                    for x in range(PAIR)
                ]
                queries = jnp.concatenate([q_buf[:, at] for at in heads], axis=0)
                grads = jnp.concatenate([do_buf[:, at] for at in heads], axis=0)
                mask = bias[...]
                scores = matmul(keys, queries, (1, 1)) + jnp.concatenate([mask] * PAIR, axis=1)
                highest = jnp.max(scores, axis=0, keepdims=True)
                weights = jnp.exp2((scores - highest) * exponent)
                weights = weights * (1.0 / jnp.sum(weights, axis=0, keepdims=True))
                low = weights.astype(jnp.bfloat16)
                attended = matmul(values_t, low, (1, 0)).T.astype(jnp.bfloat16)
                prob_grads = matmul(values, grads, (1, 1))
                delta = jnp.sum(weights * prob_grads, axis=0, keepdims=True)
                score_grads = (weights * (prob_grads - delta)).astype(jnp.bfloat16)
                query_grad = (matmul(keys_t, score_grads, (1, 0)) * score_scale).T
                query_grad = query_grad.astype(jnp.bfloat16)
                for x, at in enumerate(heads):
                    out_buf[:, at] = attended[x * rows : (x + 1) * rows]
                    dq_buf[:, at] = query_grad[x * rows : (x + 1) * rows]
                more_keys = matmul(score_grads, queries, (1, 0))
                more_values = matmul(low, grads, (1, 0))
                key_grad = more_keys if key_grad is None else key_grad + more_keys
                value_grad = more_values if value_grad is None else value_grad + more_values
            key_grad = key_grad * score_scale
            key_acc[:, own_at] = key_grad[:rows]
            value_acc[:, own_at] = value_grad[:rows]
            for o in range(1, n):
                owner = lax.rem(me - o + n, n)
                for grad, at in ((key_grad, base), (value_grad, base + HEAD_DIM)):
                    piece = jnp.zeros((BLK, HEAD_DIM), jnp.float32)
                    for j, block in enumerate(listed):
                        first = rows + j * BLK
                        piece = jnp.where(
                            block // own_blocks == owner, grad[first : first + BLK], piece
                        )
                    grad_send[o, c, :, at : at + HEAD_DIM] = piece.astype(jnp.bfloat16)
        for o in range(1, n):
            returns[o, c] = pltpu.make_async_remote_copy(
                src_ref=grad_send.at[o, c],
                dst_ref=grad_recv.at[o, c],
                send_sem=bwd_send.at[o, c],
                recv_sem=bwd_recv.at[o, c],
                device_id={"ctx": lax.rem(me - o + n, n)},
                device_id_type=pl.DeviceIdType.MESH,
            )
            returns[o, c].start()
        for i, (src, dst) in enumerate(((out_buf, out_hbm), (dq_buf, dq_hbm))):
            stores[i, c] = pltpu.make_async_copy(
                src.at[:, cols(c)], dst.at[:, cols(c)], store_sem.at[i, c]
            )
            stores[i, c].start()

    for c in range(CHUNKS):
        for o in range(1, n):
            returns[o, c].wait_recv()
        for i in range(PER_CHUNK):
            g = c * PER_CHUNK + i
            own_at = slice(g * HEAD_DIM, (g + 1) * HEAD_DIM)
            base = 2 * i * HEAD_DIM
            for acc, result, at in ((key_acc, dk_ref, base), (value_acc, dv_ref, base + HEAD_DIM)):
                sums = [acc[b * BLK : (b + 1) * BLK, own_at] for b in range(own_blocks)]
                for o in range(1, n):
                    peer = lax.rem(me + o, n)
                    part = grad_recv[o, c, :, at : at + HEAD_DIM].astype(jnp.float32)
                    for b in range(own_blocks):
                        hit = jnp.int32(0)
                        for j in range(listed_count):
                            hit = jnp.where(need_ref[peer, j] == me * own_blocks + b, 1, hit)
                        sums[b] = sums[b] + jnp.where(hit > 0, part, 0.0)
                for b in range(own_blocks):
                    result[b * BLK : (b + 1) * BLK, own_at] = sums[b].astype(jnp.bfloat16)
    for c in range(CHUNKS):
        for o in range(n):
            if o != side:
                fetches[o, c].wait_send()
            if o != 0:
                returns[o, c].wait_send()
        stores[0, c].wait()
        stores[1, c].wait()


def on_device(queries, key_states, value_states, grads_out, doc_lengths, block_plan, needed):
    n = lax.axis_size("ctx")
    rows, width = queries.shape
    kv_width = key_states.shape[1]
    blocked = (rows // BLK, BLK, kv_width)
    key_count = rows + needed.shape[1] * BLK
    vmem = pl.BlockSpec(memory_space=pltpu.VMEM)
    smem = pl.BlockSpec(memory_space=pltpu.SMEM)
    anywhere = pl.BlockSpec(memory_space=pl.ANY)
    wide = jax.ShapeDtypeStruct((rows, width), jnp.bfloat16)
    narrow = jax.ShapeDtypeStruct((rows, kv_width), jnp.bfloat16)
    exchange = pltpu.VMEM((n, CHUNKS, BLK, WIDE), jnp.bfloat16)
    dma = pltpu.SemaphoreType.DMA
    return pl.pallas_call(
        functools.partial(kernel, n),
        out_shape=(wide, wide, narrow, narrow),
        in_specs=[anywhere, vmem, vmem, anywhere, smem, smem, smem],
        out_specs=(anywhere, anywhere, vmem, vmem),
        scratch_shapes=[pltpu.VMEM((rows, width), jnp.bfloat16)] * 4
        + [pltpu.VMEM((rows, kv_width), jnp.float32)] * 2
        + [pltpu.VMEM((key_count, rows), jnp.float32)]
        + [exchange] * 3
        + [pltpu.VMEM((n, BLK, WIDE), jnp.bfloat16)] * CHUNKS
        + [pltpu.VMEM((rows // BLK, BLK, WIDE), jnp.bfloat16)] * CHUNKS
        + [pltpu.VMEM((CHUNKS, rows // BLK, BLK, WIDE), jnp.bfloat16)]
        + [dma((n, CHUNKS))] * 4
        + [dma((2, CHUNKS))] * 2,
        compiler_params=pltpu.CompilerParams(collective_id=0, has_side_effects=True),
    )(
        queries,
        key_states.reshape(blocked),
        value_states.reshape(blocked),
        grads_out,
        doc_lengths,
        block_plan,
        needed,
    )


def solution(mesh):
    tokens = P(("grp", "ctx"), None)
    return jax.shard_map(
        on_device,
        mesh=mesh,
        in_specs=(tokens, tokens, tokens, tokens, P("grp"), P("grp"), P("grp", None)),
        out_specs=(tokens, tokens, tokens, tokens),
        check_vma=False,
    )
```

```python
import functools
import math

import jax
import jax.numpy as jnp
from jax import lax
from jax.experimental import pallas as pl
from jax.experimental.pallas import tpu as pltpu
from jax.sharding import PartitionSpec as P

HEADS = 32
KV_HEADS = 4
HEAD_DIM = 128
BLK = 64
GROUP = HEADS // KV_HEADS
CHUNKS = 2
PER_CHUNK = KV_HEADS // CHUNKS
WIDE = 2 * HEAD_DIM * PER_CHUNK
PAIR = 2

masked_score = -1e30


def matmul(a, b, contract):
    return lax.dot_general(
        a, b, ((contract[:1], contract[1:]), ((), ())), preferred_element_type=jnp.float32
    )


def kernel(n, q_hbm, k_ref, v_ref, do_hbm, doc_ref, plan_ref, need_ref, *rest):
    out_hbm, dq_hbm, dk_ref, dv_ref = rest[:4]
    q_buf, do_buf, out_buf, dq_buf, key_acc, value_acc, bias = rest[4:11]
    send, grad_send, grad_recv = rest[11:14]
    recv = rest[14 : 14 + CHUNKS]
    relayed = rest[14 + CHUNKS : 14 + 2 * CHUNKS]
    grad_parts = rest[14 + 2 * CHUNKS : 14 + 3 * CHUNKS]
    grad_relayed = rest[14 + 3 * CHUNKS : 14 + 4 * CHUNKS]
    whole = rest[14 + 4 * CHUNKS]
    fwd_send, fwd_recv, bwd_send, bwd_recv, load_sem, store_sem = rest[15 + 4 * CHUNKS :]
    rows = q_buf.shape[0]
    own_blocks = rows // BLK
    listed_count = need_ref.shape[1]
    me = lax.axis_index("ctx")
    side = n // 2
    local = lax.rem(me, side)
    side_start = me - local
    partner = lax.rem(me + side, n)
    score_scale = 1.0 / math.sqrt(HEAD_DIM)
    chunk_cols = PER_CHUNK * GROUP * HEAD_DIM

    def cols(c):
        return pl.ds(c * chunk_cols, chunk_cols)

    loads, stores, fetches, returns = {}, {}, {}, {}
    for c in range(CHUNKS):
        for i, (src, dst) in enumerate(((q_hbm, q_buf), (do_hbm, do_buf))):
            loads[i, c] = pltpu.make_async_copy(
                src.at[:, cols(c)], dst.at[:, cols(c)], load_sem.at[i, c]
            )
            loads[i, c].start()

    barrier = pltpu.get_barrier_semaphore()
    for o in range(1, n):
        pl.semaphore_signal(
            barrier,
            inc=1,
            device_id={"ctx": lax.rem(me + o, n)},
            device_id_type=pl.DeviceIdType.MESH,
        )

    def near(o):
        return side_start + lax.rem(local + o, side)

    def half_for(peer, owner):
        half = jnp.int32(0)
        for j in range(listed_count):
            block = need_ref[peer, j]
            half = jnp.where(block // own_blocks == owner, block % own_blocks, half)
        return half

    def pack(keys, values, c):
        pieces = []
        for i in range(PER_CHUNK):
            g = c * PER_CHUNK + i
            at = slice(g * HEAD_DIM, (g + 1) * HEAD_DIM)
            pieces += [keys[:, at], values[:, at]]
        return jnp.concatenate(pieces, axis=1)

    def fetch(key, src, dst, peer, slot, c):
        fetches[key] = pltpu.make_async_remote_copy(
            src_ref=src,
            dst_ref=dst,
            send_sem=fwd_send.at[slot, c],
            recv_sem=fwd_recv.at[slot, c],
            device_id={"ctx": peer},
            device_id_type=pl.DeviceIdType.MESH,
        )
        fetches[key].start()

    for c in range(CHUNKS):
        for b in range(own_blocks):
            whole[c, b] = pack(k_ref[b], v_ref[b], c)
    for o in range(1, side):
        half = half_for(near(o), me)
        keys, values = k_ref[half], v_ref[half]
        for c in range(CHUNKS):
            send[o, c] = pack(keys, values, c)
    for c in range(CHUNKS):
        recv[c][0] = jnp.zeros((BLK, WIDE), jnp.bfloat16)

    pl.semaphore_wait(barrier, n - 1)
    for c in range(CHUNKS):
        fetch((0, c), whole.at[c], relayed[c], partner, 0, c)
    for c in range(CHUNKS):
        for o in range(1, side):
            fetch((o, c), send.at[o, c], recv[c].at[o], near(o), o, c)

    ends, total = [], jnp.int32(0)
    for d in range(doc_ref.shape[0]):
        total = total + doc_ref[d]
        ends.append(total)

    def documents(place):
        doc = jnp.zeros_like(place)
        for end in ends:
            doc = doc + (place >= end).astype(jnp.int32)
        return doc

    key_row = lax.broadcasted_iota(jnp.int32, (BLK, rows), 0)
    query_col = lax.broadcasted_iota(jnp.int32, (BLK, rows), 1)
    query_local = query_col // BLK
    query_place = query_col
    for b in range(own_blocks):
        shift = (plan_ref[me * own_blocks + b] - b) * BLK
        query_place = jnp.where(query_local == b, query_col + shift, query_place)
    query_doc = documents(query_place)
    listed = [need_ref[me, j] for j in range(listed_count)]
    for s in range(own_blocks + listed_count):
        if s < own_blocks:
            block = me * own_blocks + s
            found = jnp.int32(0)
            for b in listed:
                found = jnp.where(b == block, 1, found)
            allowed = jnp.where(query_local == s, 1, found)
        else:
            block = listed[s - own_blocks]
            allowed = jnp.where(block // own_blocks == me, 0, jnp.ones_like(query_col))
        key_place = key_row + plan_ref[block] * BLK
        visible = (allowed > 0) & (documents(key_place) == query_doc) & (key_place <= query_place)
        bias[s * BLK : (s + 1) * BLK, :] = jnp.where(visible, 0.0, masked_score)

    for c in range(CHUNKS):
        fetches[0, c].wait_recv()
        for o in range(1, side):
            send[side + o, c] = relayed[c][half_for(near(o), partner)]
            fetch((side + o, c), send.at[side + o, c], recv[c].at[side + o], near(o), side + o, c)
        recv[c][side] = relayed[c][half_for(me, partner)]

    def part_for(requester, owner):
        part = jnp.int32(0)
        for j in range(listed_count):
            part = jnp.where(need_ref[requester, j] // own_blocks == owner, j, part)
        return part

    def send_back(key, src, dst, peer, slot, c):
        returns[key] = pltpu.make_async_remote_copy(
            src_ref=src,
            dst_ref=dst,
            send_sem=bwd_send.at[slot, c],
            recv_sem=bwd_recv.at[slot, c],
            device_id={"ctx": peer},
            device_id_type=pl.DeviceIdType.MESH,
        )
        returns[key].start()

    slots = []
    for b in listed:
        owner = b // own_blocks
        owner_local = owner % side
        apart = jnp.where(owner - owner_local == side_start, 0, side)
        slots.append(lax.rem(local - owner_local + side, side) + apart)
    exponent = score_scale * math.log2(math.e)

    for c in range(CHUNKS):
        loads[0, c].wait()
        loads[1, c].wait()
        for o in range(1, n):
            if o != side:
                fetches[o, c].wait_recv()
        arrived = [recv[c][slot] for slot in slots]
        for i in range(PER_CHUNK):
            g = c * PER_CHUNK + i
            own_at = slice(g * HEAD_DIM, (g + 1) * HEAD_DIM)
            base = 2 * i * HEAD_DIM
            keys = jnp.concatenate(
                [k_ref[b, :, own_at] for b in range(own_blocks)]
                + [piece[:, base : base + HEAD_DIM] for piece in arrived],
                axis=0,
            )
            values = jnp.concatenate(
                [v_ref[b, :, own_at] for b in range(own_blocks)]
                + [piece[:, base + HEAD_DIM : base + 2 * HEAD_DIM] for piece in arrived],
                axis=0,
            )
            keys_t, values_t = keys.T, values.T
            key_grad = value_grad = None
            for p in range(GROUP // PAIR):
                heads = [
                    slice((g * GROUP + p * PAIR + x) * HEAD_DIM, (g * GROUP + p * PAIR + x + 1) * HEAD_DIM)
                    for x in range(PAIR)
                ]
                queries = jnp.concatenate([q_buf[:, at] for at in heads], axis=0)
                grads = jnp.concatenate([do_buf[:, at] for at in heads], axis=0)
                mask = bias[...]
                scores = matmul(keys, queries, (1, 1)) + jnp.concatenate([mask] * PAIR, axis=1)
                highest = jnp.max(scores, axis=0, keepdims=True)
                weights = jnp.exp2((scores - highest) * exponent)
                weights = weights * (1.0 / jnp.sum(weights, axis=0, keepdims=True))
                low = weights.astype(jnp.bfloat16)
                attended = matmul(values_t, low, (1, 0)).T.astype(jnp.bfloat16)
                prob_grads = matmul(values, grads, (1, 1))
                delta = jnp.sum(weights * prob_grads, axis=0, keepdims=True)
                score_grads = (weights * (prob_grads - delta)).astype(jnp.bfloat16)
                query_grad = (matmul(keys_t, score_grads, (1, 0)) * score_scale).T
                query_grad = query_grad.astype(jnp.bfloat16)
                for x, at in enumerate(heads):
                    out_buf[:, at] = attended[x * rows : (x + 1) * rows]
                    dq_buf[:, at] = query_grad[x * rows : (x + 1) * rows]
                more_keys = matmul(score_grads, queries, (1, 0))
                more_values = matmul(low, grads, (1, 0))
                key_grad = more_keys if key_grad is None else key_grad + more_keys
                value_grad = more_values if value_grad is None else value_grad + more_values
            key_grad = key_grad * score_scale
            key_acc[:, own_at] = key_grad[:rows]
            value_acc[:, own_at] = value_grad[:rows]
            for grad, at in ((key_grad, base), (value_grad, base + HEAD_DIM)):
                for j in range(listed_count):
                    first = rows + j * BLK
                    grad_parts[c][j, :, at : at + HEAD_DIM] = grad[first : first + BLK].astype(
                        jnp.bfloat16
                    )
        send_back((0, c), grad_parts[c], grad_relayed[c], partner, 0, c)
        for o in range(1, side):
            owner = near(side - o)
            grad_send[o, c] = grad_parts[c][part_for(me, owner)]
            send_back((o, c), grad_send.at[o, c], grad_recv.at[o, c], owner, o, c)
        for i, (src, dst) in enumerate(((out_buf, out_hbm), (dq_buf, dq_hbm))):
            stores[i, c] = pltpu.make_async_copy(
                src.at[:, cols(c)], dst.at[:, cols(c)], store_sem.at[i, c]
            )
            stores[i, c].start()

    for c in range(CHUNKS):
        returns[0, c].wait_recv()
        for o in range(1, side):
            owner, slot = near(side - o), side + o
            grad_send[slot, c] = grad_relayed[c][part_for(partner, owner)]
            send_back((slot, c), grad_send.at[slot, c], grad_recv.at[slot, c], owner, slot, c)
        grad_recv[side, c] = grad_relayed[c][part_for(partner, me)]

    for c in range(CHUNKS):
        for o in range(1, n):
            if o != side:
                returns[o, c].wait_recv()
        for i in range(PER_CHUNK):
            g = c * PER_CHUNK + i
            own_at = slice(g * HEAD_DIM, (g + 1) * HEAD_DIM)
            base = 2 * i * HEAD_DIM
            for acc, result, at in ((key_acc, dk_ref, base), (value_acc, dv_ref, base + HEAD_DIM)):
                sums = [acc[b * BLK : (b + 1) * BLK, own_at] for b in range(own_blocks)]
                for o in range(1, n):
                    peer = near(o) if o < side else lax.rem(near(o - side) + side, n)
                    part = grad_recv[o, c, :, at : at + HEAD_DIM].astype(jnp.float32)
                    for b in range(own_blocks):
                        hit = jnp.int32(0)
                        for j in range(listed_count):
                            hit = jnp.where(need_ref[peer, j] == me * own_blocks + b, 1, hit)
                        sums[b] = sums[b] + jnp.where(hit > 0, part, 0.0)
                for b in range(own_blocks):
                    result[b * BLK : (b + 1) * BLK, own_at] = sums[b].astype(jnp.bfloat16)
    for c in range(CHUNKS):
        for o in range(n):
            if o != side:
                fetches[o, c].wait_send()
                returns[o, c].wait_send()
        stores[0, c].wait()
        stores[1, c].wait()


def on_device(queries, key_states, value_states, grads_out, doc_lengths, block_plan, needed):
    n = lax.axis_size("ctx")
    rows, width = queries.shape
    kv_width = key_states.shape[1]
    blocked = (rows // BLK, BLK, kv_width)
    key_count = rows + needed.shape[1] * BLK
    vmem = pl.BlockSpec(memory_space=pltpu.VMEM)
    smem = pl.BlockSpec(memory_space=pltpu.SMEM)
    anywhere = pl.BlockSpec(memory_space=pl.ANY)
    wide = jax.ShapeDtypeStruct((rows, width), jnp.bfloat16)
    narrow = jax.ShapeDtypeStruct((rows, kv_width), jnp.bfloat16)
    exchange = pltpu.VMEM((n, CHUNKS, BLK, WIDE), jnp.bfloat16)
    dma = pltpu.SemaphoreType.DMA
    return pl.pallas_call(
        functools.partial(kernel, n),
        out_shape=(wide, wide, narrow, narrow),
        in_specs=[anywhere, vmem, vmem, anywhere, smem, smem, smem],
        out_specs=(anywhere, anywhere, vmem, vmem),
        scratch_shapes=[pltpu.VMEM((rows, width), jnp.bfloat16)] * 4
        + [pltpu.VMEM((rows, kv_width), jnp.float32)] * 2
        + [pltpu.VMEM((key_count, rows), jnp.float32)]
        + [exchange] * 3
        + [pltpu.VMEM((n, BLK, WIDE), jnp.bfloat16)] * CHUNKS
        + [pltpu.VMEM((rows // BLK, BLK, WIDE), jnp.bfloat16)] * CHUNKS
        + [pltpu.VMEM((needed.shape[1], BLK, WIDE), jnp.bfloat16)] * (2 * CHUNKS)
        + [pltpu.VMEM((CHUNKS, rows // BLK, BLK, WIDE), jnp.bfloat16)]
        + [dma((n, CHUNKS))] * 4
        + [dma((2, CHUNKS))] * 2,
        compiler_params=pltpu.CompilerParams(collective_id=0, has_side_effects=True),
    )(
        queries,
        key_states.reshape(blocked),
        value_states.reshape(blocked),
        grads_out,
        doc_lengths,
        block_plan,
        needed,
    )


def solution(mesh):
    tokens = P(("grp", "ctx"), None)
    return jax.shard_map(
        on_device,
        mesh=mesh,
        in_specs=(tokens, tokens, tokens, tokens, P("grp"), P("grp"), P("grp", None)),
        out_specs=(tokens, tokens, tokens, tokens),
        check_vma=False,
    )
```
